128 devices in a mesh: gz: 128 (over y, z, x, core).
Axes of the slice: x: 4, y: 4, z: 4, core: 2. Of those that a mesh axis runs over, the one named last changes fastest.
Arguments:
- scores: int32 [512, 512, 512], P('gz'), may hold values from 0 to 134217727, as said below
Outputs:
- status: int32 [512, 512, 512], P('gz')
- counts: int32 [3], replicated
The draws below stay inside these ranges and needn't reach their ends.
Inputs may be any that keep to these rules, and one draw needn't show every extreme that they name: `scores`: all values distinct: a permutation of 0 to 134217727.
All inputs are finite; a program needn't handle non-finite values.
Results may differ from the reference program's by a relative error of at most 0.000001.
Values may be sent and summed in bfloat16 or wider, within the bound.
A program may use at most 64 MiB of HBM per device.

```python
import jax
import jax.numpy as jnp

NX = 512
NY = 512
ROUNDS = 3
NZ = 512


def draw_scores(key, part):
    return jax.random.permutation(key, NX * NY * NZ).astype(jnp.int32).reshape(NZ, NX, NY)


def setup_inputs(seed: int = 0) -> dict:
    splits = jax.random.split(jax.random.key(seed), 2)
    return {
        "scores": draw_scores(jax.random.fold_in(splits[1], 71), 0),
    }


ceiling = 1 << 30


def lateral_max(field):
    padded = jnp.pad(field, ((0, 0), (1, 1), (1, 1)))
    rows_max = jnp.maximum(jnp.maximum(padded[:, :-2, :], padded[:, 1:-1, :]), padded[:, 2:, :])
    return jnp.maximum(jnp.maximum(rows_max[:, :, :-2], rows_max[:, :, 1:-1]), rows_max[:, :, 2:])


def box_maximum(extended):
    depth_max = jnp.maximum(jnp.maximum(extended[:-2], extended[1:-1]), extended[2:])
    return lateral_max(depth_max)


def reference(scores):
    status = jnp.zeros(scores.shape, jnp.int32)
    totals = []
    for round_index in range(ROUNDS):
        labels = jnp.where(status == 0, 4 * scores + 4, jnp.where(status == 1, ceiling, 0)).astype(jnp.int32)
        near_max = box_maximum(jnp.pad(labels, ((1, 1), (0, 0), (0, 0))))
        far_max = box_maximum(jnp.pad(near_max, ((1, 1), (0, 0), (0, 0))))
        undecided = status == 0
        status = jnp.where(undecided & (far_max >= ceiling), 2,
                           jnp.where(undecided & (far_max == labels), 1, status)).astype(jnp.int32)
        totals.append(jnp.sum((status == 0).astype(jnp.int32)).astype(jnp.int32))
    return status, jnp.stack(totals).astype(jnp.int32)
```

```python
import functools
import math

import jax
import jax.numpy as jnp
from jax import lax
from jax.experimental import pallas as pl
from jax.experimental.pallas import tpu as pltpu
from jax.sharding import PartitionSpec as P


AXIS = "gz"
SUB = 8
LANES = 128
PARTS = 4
HALO = 2
GROUP = 8
JUDGED = 4
WIDENED = 8
LOW = 0x0C
HIGH = 0x30


def roll(x, shift, axis):
    return pltpu.roll(x, shift % x.shape[axis], axis)


def lane_index():
    return lax.broadcasted_iota(jnp.int32, (SUB, LANES), 1)


def encode(score):
    value = ((score & ((1 << 23) - 1)) | (1 << 23)).astype(jnp.float32)
    scale = lax.shift_left(jnp.ones_like(score), lax.shift_right_logical(score, 23))
    return value * scale.astype(jnp.float32)


def lanes5(x, op, lane):
    blank = jnp.zeros_like(x[0])
    low, high = op(x[0], x[1]), op(x[2], x[3])
    whole = op(low, high)

    def before(v):
        return jnp.where(lane == 0, blank, roll(v, 1, 1))

    def after(v):
        return jnp.where(lane == LANES - 1, blank, roll(v, -1, 1))

    return [
        op(op(low, x[2]), before(high)),
        op(whole, before(x[3])),
        op(whole, after(x[0])),
        op(op(x[1], high), after(low)),
    ]


def rows5(load, op):
    x = {d: load(d) for d in range(-2, 6)}
    middle = op(x[1], x[2])
    left, right = op(x[0], middle), op(middle, x[3])
    left, right = op(x[-1], left), op(right, x[4])
    return [op(left, x[-2]), op(left, x[3]), op(x[0], right), op(right, x[5])]


def kernel(
    n, scores, packed_status, counts, raw, turned, codes, field, wide, near, bits,
    reach, found, status, cand_send, cand_recv, resp_send, resp_recv, tally, cnt_send, cnt_mid,
    recv_a, recv_b, in_sem, send_sem, recv_sem, sem_a, sem_b,
):
    depth, nx, ny = scores.shape
    chunks = ny // LANES
    steps = nx // SUB
    part_steps = steps // PARTS
    part_pairs = part_steps // 2
    group = math.gcd(GROUP, n)
    blocks = n // group
    me = lax.axis_index(AXIS)
    has = (me > 0, me < n - 1)
    lone = tuple(jnp.where(h, 0, 1).astype(jnp.int32) for h in has)
    columns = [slice(c * LANES, (c + 1) * LANES) for c in range(chunks)]

    def fetch(piece, z):
        return pltpu.make_async_copy(
            scores.at[z, :, columns[piece]], raw.at[piece, z], in_sem.at[piece, z]
        )

    for piece in range(chunks):
        for z in range(depth):
            fetch(piece, z).start()

    barrier = pltpu.get_barrier_semaphore()

    def greet(device):
        pl.semaphore_signal(
            barrier, inc=1, device_id=(device,), device_id_type=pl.DeviceIdType.MESH
        )

    place = lax.rem(me, group)
    base = me - place

    @pl.loop(1, group)
    def _(i):
        greet(base + lax.rem(place + i, group))

    @pl.loop(1, blocks)
    def _(i):
        greet(lax.rem(me + i * group, n))

    outside = (has[0] & (place == 0), has[1] & (place == group - 1))
    for side in range(2):

        @pl.when(outside[side])
        def _():
            greet(me + (1 if side else -1))

    tally[...] = jnp.zeros_like(tally)
    for side, mask in ((0, LOW), (1, HIGH)):

        @pl.when(jnp.logical_not(has[side]))
        def _():
            for phase in range(2):
                cand_recv[phase, side] = jnp.zeros(cand_recv.shape[2:], jnp.int32)
                resp_recv[phase, side] = jnp.full(
                    resp_recv.shape[2:], mask | mask << 16, jnp.int32
                )

    def wrap(ref, index):
        row = lax.broadcasted_iota(jnp.int32, (SUB, ny), 0)
        zero = jnp.zeros((SUB, ny), ref.dtype)
        for d in range(HALO):
            above = ref[index + (steps + d,)]
            ref[index + (d,)] = jnp.where(row == 0, zero, roll(above, 1, 0))
            below = ref[index + (HALO + d,)]
            ref[index + (HALO + steps + d,)] = jnp.where(
                row == SUB - 1, zero, roll(below, -1, 0)
            )

    def exchange(send, recv, phase, step, side, part, arrival):
        rows = pl.ds(part * part_pairs, part_pairs)
        there = arrival if arrival is not None else 1 - side
        return pltpu.make_async_remote_copy(
            src_ref=send.at[phase, side, rows],
            dst_ref=recv.at[phase, there, rows],
            send_sem=send_sem.at[step, side, part],
            recv_sem=recv_sem.at[step, there, part],
            device_id=(me + (1 if side else -1),),
            device_id_type=pl.DeviceIdType.MESH,
        )

    def start(send, recv, phase, step, part):
        for side in range(2):

            @pl.when(has[side])
            def _():
                exchange(send, recv, phase, step, side, part, None).start()

    def finish(send, recv, phase, step, part):
        for side in range(2):

            @pl.when(has[side])
            def _():
                exchange(send, recv, phase, step, side, part, None).wait_send()
                exchange(send, recv, phase, step, side, part, side).wait_recv()

    def turn(piece):
        for z in range(depth):
            for c in range(chunks):
                block = raw[piece, z, pl.ds(c, LANES, stride=chunks), :].T
                for half in range(LANES // steps):
                    turned[
                        z, c, pl.ds(piece * (LANES // steps) + half, steps, stride=SUB), :
                    ] = block[half * steps : (half + 1) * steps]

    def spot(c, k, z):
        return 8 + 4 * (c % 2) + 2 * (k % 2) + z % 2

    def widen(i):
        lane = lane_index()
        k = WIDENED * i
        for r in range(WIDENED):
            for z in range(depth):
                row = []
                for c in range(chunks):
                    score = turned[
                        z, c, pl.ds(pl.multiple_of(SUB * k, SUB) + SUB * r, SUB), :
                    ]
                    codes[z, k + r, :, columns[c]] = (score << 4) | spot(c, r, z)
                    value = encode(score)
                    field[z, k + r, :, columns[c]] = value
                    row.append(value)
                for c, v in enumerate(lanes5(row, jnp.maximum, lane)):
                    wide[z, k + (HALO + r), :, columns[c]] = v

    def search(phase, part):
        @pl.loop(0, part_pairs // 2)
        def _(i):
            k = part * part_steps + 4 * i
            small = [[[], []], [[], []]]
            for c in range(chunks):
                tall = [
                    rows5(lambda d: wide[z, k + (HALO + d), :, columns[c]], jnp.maximum)
                    for z in range(depth)
                ]
                best_code = ([], [])
                for r in range(4):
                    w = [tall[z][r] for z in range(depth)]
                    low, high = jnp.maximum(w[0], w[1]), jnp.maximum(w[2], w[3])
                    near[0, 0, k + r, :, columns[c]] = w[0]
                    near[0, 1, k + r, :, columns[c]] = low
                    near[1, 0, k + r, :, columns[c]] = high
                    near[1, 1, k + r, :, columns[c]] = w[3]
                    whole = jnp.maximum(low, high)
                    peak = [jnp.maximum(low, w[2]), whole, whole, jnp.maximum(w[1], high)]
                    best = [
                        field[z, k + r, :, columns[c]] == peak[z] for z in range(depth)
                    ]
                    own = [jnp.where(best[z], 4 << z, 0) for z in range(depth)]
                    found[k + r, :, columns[c]] = (own[0] | own[1]) | (own[2] | own[3])
                    for side in range(2):
                        a, b = 2 * side, 2 * side + 1
                        best_code[side].append(
                            jnp.where(
                                best[a],
                                codes[a, k + r, :, columns[c]],
                                jnp.where(best[b], codes[b, k + r, :, columns[c]], 0),
                            )
                        )
                for side in range(2):
                    for half in range(2):
                        small[side][half].append(
                            jnp.maximum(
                                best_code[side][2 * half], best_code[side][2 * half + 1]
                            )
                        )
            count = jnp.zeros((SUB, LANES), jnp.int32)
            for side in range(2):
                for half in range(2):
                    for c in range(chunks // 2):
                        v = jnp.maximum(*small[side][half][2 * c : 2 * c + 2])
                        cand_send[
                            phase, side, part * part_pairs + 2 * i + half, :, columns[c]
                        ] = v
                        if phase:
                            count = count + jnp.where(v > 0, lone[side], 0)
            if phase:
                tally[2] += count

    def judge(phase, part):
        @pl.loop(0, part_pairs // JUDGED)
        def _(i):
            count = jnp.zeros((SUB, LANES), jnp.int32)
            first = part * part_pairs + JUDGED * i
            for j in range(JUDGED):
                k = 2 * first + 2 * j
                halo = [[0] * chunks, [0] * chunks]
                for side, answer in ((0, HIGH), (1, LOW)):
                    verdicts = []
                    for p in range(chunks // 2):
                        code = cand_recv[phase, side, first + j, :, columns[p]]
                        plane = (code & 1) != 0
                        row = (code & 2) != 0
                        odd = (code & 4) != 0
                        bar = [
                            [
                                jnp.where(
                                    plane,
                                    near[side, 1, k + r, :, columns[2 * p + c]],
                                    near[side, 0, k + r, :, columns[2 * p + c]],
                                )
                                for r in range(2)
                            ]
                            for c in range(2)
                        ]
                        bar = [jnp.where(row, b[1], b[0]) for b in bar]
                        alive = (encode(code >> 4) > jnp.where(odd, bar[1], bar[0])) & (
                            code > 0
                        )
                        verdicts.append(jnp.where(alive, answer, 0))
                        if phase:
                            count = count + jnp.where(alive, 1, 0)
                            continue
                        bit = jnp.where(
                            alive, jnp.where(plane, 2 << (6 * side), 1 << (6 * side)), 0
                        )
                        for c, half in enumerate(
                            (jnp.where(odd, 0, bit), jnp.where(odd, bit, 0))
                        ):
                            halo[0][2 * p + c] |= jnp.where(row, 0, half)
                            halo[1][2 * p + c] |= jnp.where(row, half, 0)
                    resp_send[phase, side, first + j] = verdicts[0] | (verdicts[1] << 16)
                if not phase:
                    for r in range(2):
                        for c in range(chunks):
                            bits[k + r, :, columns[c]] = halo[r][c]
            if phase:
                tally[2] += count

    def allowed(phase, pair):
        word = resp_recv[phase, 0, pair] | resp_recv[phase, 1, pair]
        return word & 0xFFFF, word >> 16

    def settle(part):
        @pl.loop(0, part_pairs // JUDGED)
        def _(i):
            lane = lane_index()
            first = part * part_pairs + JUDGED * i
            for j in range(JUDGED):
                masks = allowed(0, first + j)
                for r in range(2):
                    k = 2 * first + (2 * j + r)
                    row = []
                    for c in range(chunks):
                        row.append(
                            bits[k, :, columns[c]] | (found[k, :, columns[c]] & masks[c // 2])
                        )
                        bits[k, :, columns[c]] = row[c]
                    for c, v in enumerate(lanes5(row, jnp.bitwise_or, lane)):
                        reach[k + HALO, :, columns[c]] = v

    def remove(part):
        @pl.loop(0, part_pairs // 2)
        def _(i):
            lane = lane_index()
            k = part * part_steps + 4 * i
            tall = [
                rows5(lambda d: reach[k + (HALO + d), :, columns[c]], jnp.bitwise_or)
                for c in range(chunks)
            ]
            first, second = tally[0], tally[1]
            for r in range(4):
                rows = [[] for _ in range(depth)]
                for c in range(chunks):
                    own = bits[k + r, :, columns[c]] & (LOW | HIGH)
                    held = tall[c][r]
                    two = held | (held >> 1)
                    cover = (two | (two >> 2) | (held >> 4)) & 15
                    status[c, pl.ds(pl.multiple_of(SUB * k, SUB) + SUB * r, SUB), :] = cover | (
                        own << 2
                    )
                    first = first + lax.population_count(own)
                    second = second + lax.population_count(cover)
                    for z in range(depth):
                        gone = (cover & (1 << z)) != 0
                        value = jnp.where(gone, 0.0, field[z, k + r, :, columns[c]])
                        field[z, k + r, :, columns[c]] = value
                        codes[z, k + r, :, columns[c]] = jnp.where(
                            gone, 0, codes[z, k + r, :, columns[c]]
                        )
                        rows[z].append(value)
                for z in range(depth):
                    for c, v in enumerate(lanes5(rows[z], jnp.maximum, lane)):
                        wide[z, k + (HALO + r), :, columns[c]] = v
            tally[0] = first
            tally[1] = second

    def final(part):
        @pl.loop(0, part_pairs // JUDGED)
        def _(i):
            first = part * part_pairs + JUDGED * i
            for j in range(JUDGED):
                masks = allowed(1, first + j)
                for r in range(2):
                    k = 2 * first + (2 * j + r)
                    for c in range(chunks):
                        at = pl.ds(pl.multiple_of(SUB * k, SUB), SUB)
                        held = status[c, at, :]
                        late = ((found[k, :, columns[c]] & masks[c // 2]) << 2) & ~(held << 4)
                        root = ((held | late) >> 4) & 15
                        both = root | ((held & 15 & ~root) << 8)
                        both = (both | (both << 2)) & 0x3333
                        both = (both | (both << 1)) & 0x5555
                        status[c, at, :] = (both & 0xFF) | (both >> 7)

    def offer(phase, part):
        search(phase, part)
        start(cand_send, cand_recv, phase, 2 * phase, part)

    def answer(phase, part):
        finish(cand_send, cand_recv, phase, 2 * phase, part)
        judge(phase, part)
        start(resp_send, resp_recv, phase, 2 * phase + 1, part)

    def confirm(part):
        finish(resp_send, resp_recv, 0, 1, part)
        settle(part)

    @pl.loop(0, chunks)
    def _(piece):
        for z in range(depth):
            pltpu.make_async_copy(
                scores.at[z, :, columns[0]], raw.at[piece, z], in_sem.at[piece, z]
            ).wait()
        turn(piece)

    @pl.loop(0, steps // WIDENED)
    def _(i):
        widen(i)

    for z in range(depth):
        wrap(wide, (z,))

    pl.semaphore_wait(
        barrier,
        group
        + blocks
        - 2
        + outside[0].astype(jnp.int32)
        + outside[1].astype(jnp.int32),
    )

    @pl.loop(1, PARTS + 1)
    def _(part):
        offer(0, lax.rem(part, PARTS))

    @pl.loop(1, PARTS + 1)
    def _(part):
        answer(0, lax.rem(part, PARTS))

    @pl.loop(1, PARTS)
    def _(part):
        confirm(part)

    remove(2)
    confirm(0)
    wrap(reach, ())

    @pl.loop(3, 6)
    def _(part):
        remove(lax.rem(part, PARTS))

    for z in range(depth):
        wrap(wide, (z,))

    @pl.loop(3, PARTS + 3)
    def _(part):
        offer(1, lax.rem(part, PARTS))

    @pl.loop(3, PARTS + 3)
    def _(part):
        answer(1, lax.rem(part, PARTS))

    roots, covered, late = (jnp.sum(tally[i]) for i in range(3))
    cells = depth * nx * ny
    column = lax.broadcasted_iota(jnp.int32, (1, LANES), 1)
    mine = jnp.where(
        column == 0,
        cells - roots,
        jnp.where(column == 1, cells - covered, cells - covered - late),
    )
    cnt_send[...] = mine

    def gather(send, recv, sems, i, device):
        return pltpu.make_async_remote_copy(
            src_ref=send,
            dst_ref=recv.at[i],
            send_sem=sems.at[0, i],
            recv_sem=sems.at[1, i],
            device_id=(device,),
            device_id_type=pl.DeviceIdType.MESH,
        )

    def near_by(i):
        return gather(cnt_send, recv_a, sem_a, i, base + lax.rem(place + i, group))

    def far_off(i):
        return gather(cnt_mid, recv_b, sem_b, i, lax.rem(me + i * group, n))

    @pl.loop(1, group)
    def _(i):
        near_by(i).start()

    def present(c):
        for piece in range(chunks):
            block = jnp.concatenate(
                [
                    status[
                        c, pl.ds(piece * (LANES // steps) + half, steps, stride=SUB), :
                    ]
                    for half in range(LANES // steps)
                ],
                axis=0,
            )
            packed_status[piece, pl.ds(c, LANES, stride=chunks), :] = block.T

    @pl.loop(1, group)
    def _(i):
        near_by(i).wait()

    subtotal = mine
    for i in range(1, group):
        subtotal = subtotal + recv_a[i]
    cnt_mid[...] = subtotal

    @pl.loop(1, blocks)
    def _(i):
        far_off(i).start()

    @pl.loop(3, PARTS + 3)
    def _(part):
        part = lax.rem(part, PARTS)
        finish(resp_send, resp_recv, 1, 3, part)
        final(part)

    for c in range(chunks):
        present(c)

    @pl.loop(1, blocks)
    def _(i):
        far_off(i).wait()

    total = subtotal
    for i in range(1, blocks):
        total = total + recv_b[i]
    counts[...] = total


def shards(scores):
    depth, nx, ny = scores.shape
    n = lax.axis_size(AXIS)
    group = math.gcd(GROUP, n)
    vmem = pltpu.VMEM
    steps = nx // SUB
    pairs = steps // 2
    packed_status, counts = pl.pallas_call(
        functools.partial(kernel, n),
        out_shape=(
            jax.ShapeDtypeStruct((ny // LANES, nx, LANES), jnp.int32),
            jax.ShapeDtypeStruct((1, LANES), jnp.int32),
        ),
        in_specs=[pl.BlockSpec(memory_space=pltpu.HBM)],
        out_specs=(pl.BlockSpec(memory_space=vmem),) * 2,
        scratch_shapes=[
            vmem((ny // LANES, depth, nx, LANES), jnp.int32),
            vmem((depth, ny // LANES, nx, LANES), jnp.int32),
            vmem((depth, steps, SUB, ny), jnp.int32),
            vmem((depth, steps, SUB, ny), jnp.float32),
            vmem((depth, steps + 2 * HALO, SUB, ny), jnp.float32),
            vmem((2, 2, steps, SUB, ny), jnp.float32),
            vmem((steps, SUB, ny), jnp.int32),
            vmem((steps + 2 * HALO, SUB, ny), jnp.int32),
            vmem((steps, SUB, ny), jnp.int32),
            vmem((ny // LANES, nx, LANES), jnp.int32),
            vmem((2, 2, pairs, SUB, ny // 2), jnp.int32),
            vmem((2, 2, pairs, SUB, ny // 2), jnp.int32),
            vmem((2, 2, pairs, SUB, ny // 4), jnp.int32),
            vmem((2, 2, pairs, SUB, ny // 4), jnp.int32),
            vmem((3, SUB, LANES), jnp.int32),
            vmem((1, LANES), jnp.int32),
            vmem((1, LANES), jnp.int32),
            vmem((group, 1, LANES), jnp.int32),
            vmem((n // group, 1, LANES), jnp.int32),
            pltpu.SemaphoreType.DMA((ny // LANES, depth)),
            pltpu.SemaphoreType.DMA((4, 2, PARTS)),
            pltpu.SemaphoreType.DMA((4, 2, PARTS)),
            pltpu.SemaphoreType.DMA((2, group)),
            pltpu.SemaphoreType.DMA((2, n // group)),
        ],
        compiler_params=pltpu.CompilerParams(
            collective_id=0, has_side_effects=True, vmem_limit_bytes=61 * 1024 * 1024
        ),
    )(scores)
    place = 2 * jnp.arange(depth, dtype=jnp.int32)[:, None, None]
    flat = jnp.concatenate([packed_status[p] for p in range(ny // LANES)], axis=1)
    return (flat[None] >> place) & 3, counts[0, :3]


def solution(mesh):
    return jax.shard_map(
        shards,
        mesh=mesh,
        in_specs=(P(AXIS, None, None),),
        out_specs=(P(AXIS, None, None), P()),
        check_vma=False,
    )
```

```python
import functools
import math

import jax
import jax.numpy as jnp
from jax import lax
from jax.experimental import pallas as pl
from jax.experimental.pallas import tpu as pltpu
from jax.sharding import PartitionSpec as P


AXIS = "gz"
SUB = 8
LANES = 128
PARTS = 8
HALO = 2
GROUP = 8
JUDGED = 4
SPLIT = 32
LOW = 0x0C
HIGH = 0x30


def roll(x, shift, axis):
    return pltpu.roll(x, shift % x.shape[axis], axis)


def lane_index():
    return lax.broadcasted_iota(jnp.int32, (SUB, LANES), 1)


def encode(score):
    value = ((score & ((1 << 23) - 1)) | (1 << 23)).astype(jnp.float32)
    scale = lax.shift_left(jnp.ones_like(score), lax.shift_right_logical(score, 23))
    return value * scale.astype(jnp.float32)


def lanes5(x, op, lane):
    blank = jnp.zeros_like(x[0])
    low, high = op(x[0], x[1]), op(x[2], x[3])
    whole = op(low, high)

    def before(v):
        return jnp.where(lane == 0, blank, roll(v, 1, 1))

    def after(v):
        return jnp.where(lane == LANES - 1, blank, roll(v, -1, 1))

    return [
        op(op(low, x[2]), before(high)),
        op(whole, before(x[3])),
        op(whole, after(x[0])),
        op(op(x[1], high), after(low)),
    ]


def rows5(load, op):
    x = {d: load(d) for d in range(-2, 6)}
    middle = op(x[1], x[2])
    left, right = op(x[0], middle), op(middle, x[3])
    left, right = op(x[-1], left), op(right, x[4])
    return [op(left, x[-2]), op(left, x[3]), op(x[0], right), op(right, x[5])]


def kernel(
    n, scores, decided, counts, raw, turned, codes, field, wide, near, bits,
    reach, found, status, flat, cand_send, cand_recv, resp_send, resp_recv, tally, cnt_send, cnt_mid,
    recv_a, recv_b, in_sem, send_sem, recv_sem, sem_a, sem_b,
):
    depth, nx, ny = scores.shape
    chunks = ny // LANES
    steps = nx // SUB
    part_steps = steps // PARTS
    part_pairs = part_steps // 2
    group = math.gcd(GROUP, n)
    blocks = n // group
    me = lax.axis_index(AXIS)
    has = (me > 0, me < n - 1)
    lone = tuple(jnp.where(h, 0, 1).astype(jnp.int32) for h in has)
    columns = [slice(c * LANES, (c + 1) * LANES) for c in range(chunks)]

    def fetch(piece, z):
        return pltpu.make_async_copy(
            scores.at[z, :, columns[piece]], raw.at[piece, z], in_sem.at[piece, z]
        )

    for piece in range(chunks):
        for z in range(depth):
            fetch(piece, z).start()

    barrier = pltpu.get_barrier_semaphore()

    def greet(device):
        pl.semaphore_signal(
            barrier, inc=1, device_id=(device,), device_id_type=pl.DeviceIdType.MESH
        )

    place = lax.rem(me, group)
    base = me - place

    @pl.loop(1, group)
    def _(i):
        greet(base + lax.rem(place + i, group))

    @pl.loop(1, blocks)
    def _(i):
        greet(lax.rem(me + i * group, n))

    outside = (has[0] & (place == 0), has[1] & (place == group - 1))
    for side in range(2):

        @pl.when(outside[side])
        def _():
            greet(me + (1 if side else -1))

    tally[...] = jnp.zeros_like(tally)
    for side, mask in ((0, LOW), (1, HIGH)):

        @pl.when(jnp.logical_not(has[side]))
        def _():
            for phase in range(2):
                cand_recv[phase, side] = jnp.zeros(cand_recv.shape[2:], jnp.int32)
                resp_recv[phase, side] = jnp.full(
                    resp_recv.shape[2:], mask | mask << 16, jnp.int32
                )

    def wrap(ref, index):
        row = lax.broadcasted_iota(jnp.int32, (SUB, ny), 0)
        zero = jnp.zeros((SUB, ny), ref.dtype)
        for d in range(HALO):
            above = ref[index + (steps + d,)]
            ref[index + (d,)] = jnp.where(row == 0, zero, roll(above, 1, 0))
            below = ref[index + (HALO + d,)]
            ref[index + (HALO + steps + d,)] = jnp.where(
                row == SUB - 1, zero, roll(below, -1, 0)
            )

    def exchange(send, recv, phase, step, side, part, arrival):
        rows = pl.ds(part * part_pairs, part_pairs)
        there = arrival if arrival is not None else 1 - side
        return pltpu.make_async_remote_copy(
            src_ref=send.at[phase, side, rows],
            dst_ref=recv.at[phase, there, rows],
            send_sem=send_sem.at[step, side, part],
            recv_sem=recv_sem.at[step, there, part],
            device_id=(me + (1 if side else -1),),
            device_id_type=pl.DeviceIdType.MESH,
        )

    def start(send, recv, phase, step, part):
        for side in range(2):

            @pl.when(has[side])
            def _():
                exchange(send, recv, phase, step, side, part, None).start()

    def finish(send, recv, phase, step, part):
        for side in range(2):

            @pl.when(has[side])
            def _():
                exchange(send, recv, phase, step, side, part, None).wait_send()
                exchange(send, recv, phase, step, side, part, side).wait_recv()

    def turn(piece):
        for z in range(depth):
            for c in range(chunks):
                block = raw[piece, z, pl.ds(c, LANES, stride=chunks), :].T
                for half in range(LANES // steps):
                    turned[
                        z, c, pl.ds(piece * (LANES // steps) + half, steps, stride=SUB), :
                    ] = block[half * steps : (half + 1) * steps]

    def spot(c, k, z):
        return 8 + 4 * (c % 2) + 2 * (k % 2) + z % 2

    def widen(part):
        lane = lane_index()
        k = part * part_steps
        for r in range(part_steps):
            for z in range(depth):
                row = []
                for c in range(chunks):
                    score = turned[
                        z, c, pl.ds(pl.multiple_of(SUB * k, SUB) + SUB * r, SUB), :
                    ]
                    codes[z, k + r, :, columns[c]] = (score << 4) | spot(c, r, z)
                    value = encode(score)
                    field[z, k + r, :, columns[c]] = value
                    row.append(value)
                for c, v in enumerate(lanes5(row, jnp.maximum, lane)):
                    wide[z, k + (HALO + r), :, columns[c]] = v

    def search(phase, part):
        @pl.loop(0, part_pairs // 2)
        def _(i):
            k = part * part_steps + 4 * i
            small = [[[], []], [[], []]]
            for c in range(chunks):
                tall = [
                    rows5(lambda d: wide[z, k + (HALO + d), :, columns[c]], jnp.maximum)
                    for z in range(depth)
                ]
                best_code = ([], [])
                for r in range(4):
                    w = [tall[z][r] for z in range(depth)]
                    low, high = jnp.maximum(w[0], w[1]), jnp.maximum(w[2], w[3])
                    near[0, 0, k + r, :, columns[c]] = w[0]
                    near[0, 1, k + r, :, columns[c]] = low
                    near[1, 0, k + r, :, columns[c]] = high
                    near[1, 1, k + r, :, columns[c]] = w[3]
                    whole = jnp.maximum(low, high)
                    peak = [jnp.maximum(low, w[2]), whole, whole, jnp.maximum(w[1], high)]
                    best = [
                        field[z, k + r, :, columns[c]] == peak[z] for z in range(depth)
                    ]
                    own = [jnp.where(best[z], 4 << z, 0) for z in range(depth)]
                    found[k + r, :, columns[c]] = (own[0] | own[1]) | (own[2] | own[3])
                    for side in range(2):
                        a, b = 2 * side, 2 * side + 1
                        best_code[side].append(
                            jnp.where(
                                best[a],
                                codes[a, k + r, :, columns[c]],
                                jnp.where(best[b], codes[b, k + r, :, columns[c]], 0),
                            )
                        )
                for side in range(2):
                    for half in range(2):
                        small[side][half].append(
                            jnp.maximum(
                                best_code[side][2 * half], best_code[side][2 * half + 1]
                            )
                        )
            count = jnp.zeros((SUB, LANES), jnp.int32)
            for side in range(2):
                for half in range(2):
                    for c in range(chunks // 2):
                        v = jnp.maximum(*small[side][half][2 * c : 2 * c + 2])
                        cand_send[
                            phase, side, part * part_pairs + 2 * i + half, :, columns[c]
                        ] = v
                        if phase:
                            count = count + jnp.where(v > 0, lone[side], 0)
            if phase:
                tally[2] += count

    def judge(phase, part):
        @pl.loop(0, part_pairs // JUDGED)
        def _(i):
            count = jnp.zeros((SUB, LANES), jnp.int32)
            first = part * part_pairs + JUDGED * i
            for j in range(JUDGED):
                k = 2 * first + 2 * j
                halo = [[0] * chunks, [0] * chunks]
                for side, answer in ((0, HIGH), (1, LOW)):
                    verdicts = []
                    for p in range(chunks // 2):
                        code = cand_recv[phase, side, first + j, :, columns[p]]
                        plane = (code & 1) != 0
                        row = (code & 2) != 0
                        odd = (code & 4) != 0
                        bar = [
                            [
                                jnp.where(
                                    plane,
                                    near[side, 1, k + r, :, columns[2 * p + c]],
                                    near[side, 0, k + r, :, columns[2 * p + c]],
                                )
                                for r in range(2)
                            ]
                            for c in range(2)
                        ]
                        bar = [jnp.where(row, b[1], b[0]) for b in bar]
                        alive = (encode(code >> 4) > jnp.where(odd, bar[1], bar[0])) & (
                            code > 0
                        )
                        verdicts.append(jnp.where(alive, answer, 0))
                        if phase:
                            count = count + jnp.where(alive, 1, 0)
                            continue
                        bit = jnp.where(
                            alive, jnp.where(plane, 2 << (6 * side), 1 << (6 * side)), 0
                        )
                        for c, half in enumerate(
                            (jnp.where(odd, 0, bit), jnp.where(odd, bit, 0))
                        ):
                            halo[0][2 * p + c] |= jnp.where(row, 0, half)
                            halo[1][2 * p + c] |= jnp.where(row, half, 0)
                    resp_send[phase, side, first + j] = verdicts[0] | (verdicts[1] << 16)
                if not phase:
                    for r in range(2):
                        for c in range(chunks):
                            bits[k + r, :, columns[c]] = halo[r][c]
            if phase:
                tally[2] += count

    def allowed(phase, pair):
        word = resp_recv[phase, 0, pair] | resp_recv[phase, 1, pair]
        return word & 0xFFFF, word >> 16

    def settle(part):
        @pl.loop(0, part_pairs // JUDGED)
        def _(i):
            lane = lane_index()
            first = part * part_pairs + JUDGED * i
            for j in range(JUDGED):
                masks = allowed(0, first + j)
                for r in range(2):
                    k = 2 * first + (2 * j + r)
                    row = []
                    for c in range(chunks):
                        row.append(
                            bits[k, :, columns[c]] | (found[k, :, columns[c]] & masks[c // 2])
                        )
                        bits[k, :, columns[c]] = row[c]
                    for c, v in enumerate(lanes5(row, jnp.bitwise_or, lane)):
                        reach[k + HALO, :, columns[c]] = v

    def remove(begin, blocks_of_rows):
        @pl.loop(0, blocks_of_rows)
        def _(i):
            lane = lane_index()
            k = lax.rem(begin + 4 * i, steps)
            tall = [
                rows5(lambda d: reach[k + (HALO + d), :, columns[c]], jnp.bitwise_or)
                for c in range(chunks)
            ]
            first, second = tally[0], tally[1]
            for r in range(4):
                rows = [[] for _ in range(depth)]
                for c in range(chunks):
                    own = bits[k + r, :, columns[c]] & (LOW | HIGH)
                    held = tall[c][r]
                    two = held | (held >> 1)
                    cover = (two | (two >> 2) | (held >> 4)) & 15
                    status[c, pl.ds(pl.multiple_of(SUB * k, SUB) + SUB * r, SUB), :] = cover | (
                        own << 2
                    )
                    first = first + lax.population_count(own)
                    second = second + lax.population_count(cover)
                    for z in range(depth):
                        gone = (cover & (1 << z)) != 0
                        value = jnp.where(gone, 0.0, field[z, k + r, :, columns[c]])
                        field[z, k + r, :, columns[c]] = value
                        codes[z, k + r, :, columns[c]] = jnp.where(
                            gone, 0, codes[z, k + r, :, columns[c]]
                        )
                        rows[z].append(value)
                for z in range(depth):
                    for c, v in enumerate(lanes5(rows[z], jnp.maximum, lane)):
                        wide[z, k + (HALO + r), :, columns[c]] = v
            tally[0] = first
            tally[1] = second

    def final(part):
        @pl.loop(0, part_pairs // JUDGED)
        def _(i):
            first = part * part_pairs + JUDGED * i
            for j in range(JUDGED):
                masks = allowed(1, first + j)
                for r in range(2):
                    k = 2 * first + (2 * j + r)
                    for c in range(chunks):
                        at = pl.ds(pl.multiple_of(SUB * k, SUB), SUB)
                        held = status[c, at, :]
                        late = ((found[k, :, columns[c]] & masks[c // 2]) << 2) & ~(held << 4)
                        root = ((held | late) >> 4) & 15
                        both = root | ((held & 15 & ~root) << 8)
                        both = (both | (both << 2)) & 0x3333
                        both = (both | (both << 1)) & 0x5555
                        status[c, at, :] = (both & 0xFF) | (both >> 7)

    def offer(phase, part):
        search(phase, part)
        start(cand_send, cand_recv, phase, 2 * phase, part)

    def answer(phase, part):
        finish(cand_send, cand_recv, phase, 2 * phase, part)
        judge(phase, part)
        start(resp_send, resp_recv, phase, 2 * phase + 1, part)

    def confirm(part):
        finish(resp_send, resp_recv, 0, 1, part)
        settle(part)

    @pl.loop(0, chunks)
    def _(piece):
        for z in range(depth):
            pltpu.make_async_copy(
                scores.at[z, :, columns[0]], raw.at[piece, z], in_sem.at[piece, z]
            ).wait()
        turn(piece)

    pl.semaphore_wait(
        barrier,
        group
        + blocks
        - 2
        + outside[0].astype(jnp.int32)
        + outside[1].astype(jnp.int32),
    )

    @pl.loop(0, PARTS)
    def _(part):
        widen(part)

        @pl.when(part >= 2)
        def _():
            offer(0, part - 1)

    for z in range(depth):
        wrap(wide, (z,))

    @pl.loop(PARTS - 1, PARTS + 1)
    def _(part):
        offer(0, lax.rem(part, PARTS))

    @pl.loop(1, PARTS + 1)
    def _(part):
        answer(0, lax.rem(part, PARTS))

    @pl.loop(1, PARTS)
    def _(part):
        confirm(part)

        @pl.when(part >= 2)
        def _():
            remove(part * part_steps - 4, part_steps // 4)

        @pl.when(part >= 3)
        def _():
            offer(1, part - 1)

    confirm(0)
    wrap(reach, ())
    remove(steps - 4, part_steps // 4 + 2)
    for z in range(depth):
        wrap(wide, (z,))

    @pl.loop(PARTS - 1, PARTS + 2)
    def _(part):
        offer(1, lax.rem(part, PARTS))

    cells = depth * nx * ny
    column = lax.broadcasted_iota(jnp.int32, (1, LANES), 1)
    roots, covered = jnp.sum(tally[0]), jnp.sum(tally[1])
    mine = jnp.where(column == 0, cells - roots, cells - covered)

    @pl.loop(2, PARTS + 2)
    def _(part):
        answer(1, lax.rem(part, PARTS))

    mine = mine - jnp.where(column == 2, jnp.sum(tally[2]), 0)
    cnt_send[...] = mine

    def gather(send, recv, sems, i, device):
        return pltpu.make_async_remote_copy(
            src_ref=send,
            dst_ref=recv.at[i],
            send_sem=sems.at[0, i],
            recv_sem=sems.at[1, i],
            device_id=(device,),
            device_id_type=pl.DeviceIdType.MESH,
        )

    def near_by(i):
        return gather(cnt_send, recv_a, sem_a, i, base + lax.rem(place + i, group))

    def far_off(i):
        return gather(cnt_mid, recv_b, sem_b, i, lax.rem(me + i * group, n))

    @pl.loop(1, group)
    def _(i):
        near_by(i).start()

    def present(c):
        for piece in range(chunks):
            block = jnp.concatenate(
                [
                    status[
                        c, pl.ds(piece * (LANES // steps) + half, steps, stride=SUB), :
                    ]
                    for half in range(LANES // steps)
                ],
                axis=0,
            )
            flat[piece, pl.ds(c, LANES, stride=chunks), :] = block.T

    @pl.loop(1, group)
    def _(i):
        near_by(i).wait()

    subtotal = mine
    for i in range(1, group):
        subtotal = subtotal + recv_a[i]
    cnt_mid[...] = subtotal

    @pl.loop(1, blocks)
    def _(i):
        far_off(i).start()

    @pl.loop(2, PARTS + 2)
    def _(part):
        part = lax.rem(part, PARTS)
        finish(resp_send, resp_recv, 1, 3, part)
        final(part)

    for c in range(chunks):
        present(c)

    @pl.loop(0, nx // SPLIT)
    def _(i):
        here = pl.ds(pl.multiple_of(i * SPLIT, SPLIT), SPLIT)
        for piece in range(chunks):
            word = flat[piece, here, :]
            for z in range(depth):
                decided[z, here, columns[piece]] = (word >> (2 * z)) & 3


    @pl.loop(1, blocks)
    def _(i):
        far_off(i).wait()

    total = subtotal
    for i in range(1, blocks):
        total = total + recv_b[i]
    counts[...] = total


def shards(scores):
    depth, nx, ny = scores.shape
    n = lax.axis_size(AXIS)
    group = math.gcd(GROUP, n)
    vmem = pltpu.VMEM
    steps = nx // SUB
    pairs = steps // 2
    decided, counts = pl.pallas_call(
        functools.partial(kernel, n),
        out_shape=(
            jax.ShapeDtypeStruct((depth, nx, ny), jnp.int32),
            jax.ShapeDtypeStruct((1, LANES), jnp.int32),
        ),
        in_specs=[pl.BlockSpec(memory_space=pltpu.HBM)],
        out_specs=(pl.BlockSpec(memory_space=vmem),) * 2,
        scratch_shapes=[
            vmem((ny // LANES, depth, nx, LANES), jnp.int32),
            vmem((depth, ny // LANES, nx, LANES), jnp.int32),
            vmem((depth, steps, SUB, ny), jnp.int32),
            vmem((depth, steps, SUB, ny), jnp.float32),
            vmem((depth, steps + 2 * HALO, SUB, ny), jnp.float32),
            vmem((2, 2, steps, SUB, ny), jnp.float32),
            vmem((steps, SUB, ny), jnp.int32),
            vmem((steps + 2 * HALO, SUB, ny), jnp.int32),
            vmem((steps, SUB, ny), jnp.int32),
            vmem((ny // LANES, nx, LANES), jnp.int32),
            vmem((ny // LANES, nx, LANES), jnp.int32),
            vmem((2, 2, pairs, SUB, ny // 2), jnp.int32),
            vmem((2, 2, pairs, SUB, ny // 2), jnp.int32),
            vmem((2, 2, pairs, SUB, ny // 4), jnp.int32),
            vmem((2, 2, pairs, SUB, ny // 4), jnp.int32),
            vmem((3, SUB, LANES), jnp.int32),
            vmem((1, LANES), jnp.int32),
            vmem((1, LANES), jnp.int32),
            vmem((group, 1, LANES), jnp.int32),
            vmem((n // group, 1, LANES), jnp.int32),
            pltpu.SemaphoreType.DMA((ny // LANES, depth)),
            pltpu.SemaphoreType.DMA((4, 2, PARTS)),
            pltpu.SemaphoreType.DMA((4, 2, PARTS)),
            pltpu.SemaphoreType.DMA((2, group)),
            pltpu.SemaphoreType.DMA((2, n // group)),
        ],
        compiler_params=pltpu.CompilerParams(
            collective_id=0, has_side_effects=True, vmem_limit_bytes=48 * 1024 * 1024
        ),
    )(scores)
    return decided, counts[0, :3]


def solution(mesh):
    return jax.shard_map(
        shards,
        mesh=mesh,
        in_specs=(P(AXIS, None, None),),
        out_specs=(P(AXIS, None, None), P()),
        check_vma=False,
    )
```

```python
import functools
import math

import jax
import jax.numpy as jnp
from jax import lax
from jax.experimental import pallas as pl
from jax.experimental.pallas import tpu as pltpu
from jax.sharding import PartitionSpec as P


AXIS = "gz"
SUB = 8
LANES = 128
PARTS = 8
AHEAD = 6
HALO = 2
GROUP = 8
JUDGED = 4
SPLIT = 32
LOW = 0x0C
HIGH = 0x30
BASE = 2.0**23
PLANE = 2.0**16
ROW = 2.0**32
ODD = 2.0**64


def roll(x, shift, axis):
    return pltpu.roll(x, shift % x.shape[axis], axis)


def lane_index():
    return lax.broadcasted_iota(jnp.int32, (SUB, LANES), 1)


def encode(score):
    value = ((score & ((1 << 23) - 1)) | (1 << 23)).astype(jnp.float32)
    scale = lax.shift_left(jnp.ones_like(score), lax.shift_right_logical(score, 23))
    return value * scale.astype(jnp.float32)


def lanes5(x, op, lane):
    blank = jnp.zeros_like(x[0])
    low, high = op(x[0], x[1]), op(x[2], x[3])
    whole = op(low, high)

    def before(v):
        return jnp.where(lane == 0, blank, roll(v, 1, 1))

    def after(v):
        return jnp.where(lane == LANES - 1, blank, roll(v, -1, 1))

    return [
        op(op(low, x[2]), before(high)),
        op(whole, before(x[3])),
        op(whole, after(x[0])),
        op(op(x[1], high), after(low)),
    ]


def rows5(load, op):
    x = {d: load(d) for d in range(-2, 6)}
    middle = op(x[1], x[2])
    left, right = op(x[0], middle), op(middle, x[3])
    left, right = op(x[-1], left), op(right, x[4])
    return [op(left, x[-2]), op(left, x[3]), op(x[0], right), op(right, x[5])]


def kernel(
    n, scores, decided, counts, raw, turned, field, wide, near, bits,
    reach, found, status, flat, cand_send, cand_recv, resp_send, resp_recv, tally, cnt_send, cnt_mid,
    recv_a, recv_b, in_sem, send_sem, recv_sem, sem_a, sem_b,
):
    depth, nx, ny = scores.shape
    chunks = ny // LANES
    steps = nx // SUB
    part_steps = steps // PARTS
    part_pairs = part_steps // 2
    group = math.gcd(GROUP, n)
    blocks = n // group
    me = lax.axis_index(AXIS)
    has = (me > 0, me < n - 1)
    lone = tuple(jnp.where(h, 0, 1).astype(jnp.int32) for h in has)
    columns = [slice(c * LANES, (c + 1) * LANES) for c in range(chunks)]

    def fetch(piece, z):
        return pltpu.make_async_copy(
            scores.at[z, :, columns[piece]], raw.at[piece, z], in_sem.at[piece, z]
        )

    for piece in range(chunks):
        for z in range(depth):
            fetch(piece, z).start()

    barrier = pltpu.get_barrier_semaphore()

    def greet(device):
        pl.semaphore_signal(
            barrier, inc=1, device_id=(device,), device_id_type=pl.DeviceIdType.MESH
        )

    place = lax.rem(me, group)
    base = me - place

    @pl.loop(1, group)
    def _(i):
        greet(base + lax.rem(place + i, group))

    @pl.loop(1, blocks)
    def _(i):
        greet(lax.rem(me + i * group, n))

    outside = (has[0] & (place == 0), has[1] & (place == group - 1))
    for side in range(2):

        @pl.when(outside[side])
        def _():
            greet(me + (1 if side else -1))

    tally[...] = jnp.zeros_like(tally)
    for side, mask in ((0, LOW), (1, HIGH)):

        @pl.when(jnp.logical_not(has[side]))
        def _():
            for phase in range(2):
                cand_recv[phase, side] = jnp.zeros(cand_recv.shape[2:], jnp.float32)
                resp_recv[phase, side] = jnp.full(
                    resp_recv.shape[2:], mask | mask << 16, jnp.int32
                )

    def wrap(ref, index):
        row = lax.broadcasted_iota(jnp.int32, (SUB, ny), 0)
        zero = jnp.zeros((SUB, ny), ref.dtype)
        for d in range(HALO):
            above = ref[index + (steps + d,)]
            ref[index + (d,)] = jnp.where(row == 0, zero, roll(above, 1, 0))
            below = ref[index + (HALO + d,)]
            ref[index + (HALO + steps + d,)] = jnp.where(
                row == SUB - 1, zero, roll(below, -1, 0)
            )

    def exchange(send, recv, phase, step, side, part, arrival):
        rows = pl.ds(part * part_pairs, part_pairs)
        there = arrival if arrival is not None else 1 - side
        return pltpu.make_async_remote_copy(
            src_ref=send.at[phase, side, rows],
            dst_ref=recv.at[phase, there, rows],
            send_sem=send_sem.at[step, side, part],
            recv_sem=recv_sem.at[step, there, part],
            device_id=(me + (1 if side else -1),),
            device_id_type=pl.DeviceIdType.MESH,
        )

    def start(send, recv, phase, step, part):
        for side in range(2):

            @pl.when(has[side])
            def _():
                exchange(send, recv, phase, step, side, part, None).start()

    def finish(send, recv, phase, step, part):
        for side in range(2):

            @pl.when(has[side])
            def _():
                exchange(send, recv, phase, step, side, part, None).wait_send()
                exchange(send, recv, phase, step, side, part, side).wait_recv()

    def turn(piece):
        for z in range(depth):
            for c in range(chunks):
                block = raw[piece, z, pl.ds(c, LANES, stride=chunks), :].T
                for half in range(LANES // steps):
                    turned[
                        z, c, pl.ds(piece * (LANES // steps) + half, steps, stride=SUB), :
                    ] = block[half * steps : (half + 1) * steps]

    def widen(part):
        lane = lane_index()
        k = part * part_steps
        for r in range(part_steps):
            for z in range(depth):
                row = []
                for c in range(chunks):
                    score = turned[
                        z, c, pl.ds(pl.multiple_of(SUB * k, SUB) + SUB * r, SUB), :
                    ]
                    value = encode(score)
                    field[z, k + r, :, columns[c]] = value
                    row.append(value)
                for c, v in enumerate(lanes5(row, jnp.maximum, lane)):
                    wide[z, k + (HALO + r), :, columns[c]] = v

    def search(phase, part):
        @pl.loop(0, part_pairs // 2)
        def _(i):
            k = part * part_steps + 4 * i
            small = [[[], []], [[], []]]
            for c in range(chunks):
                tall = [
                    rows5(lambda d: wide[z, k + (HALO + d), :, columns[c]], jnp.maximum)
                    for z in range(depth)
                ]
                best_code = ([], [])
                for r in range(4):
                    w = [tall[z][r] for z in range(depth)]
                    low, high = jnp.maximum(w[0], w[1]), jnp.maximum(w[2], w[3])
                    near[0, 0, k + r, :, columns[c]] = w[0]
                    near[0, 1, k + r, :, columns[c]] = low
                    near[1, 0, k + r, :, columns[c]] = high
                    near[1, 1, k + r, :, columns[c]] = w[3]
                    whole = jnp.maximum(low, high)
                    peak = [jnp.maximum(low, w[2]), whole, whole, jnp.maximum(w[1], high)]
                    value = [field[z, k + r, :, columns[c]] for z in range(depth)]
                    best = [value[z] == peak[z] for z in range(depth)]
                    own = [
                        jnp.where(best[z], 4 << z, jnp.where(best[z + 1], 8 << z, 0))
                        for z in (0, 2)
                    ]
                    found[k + r, :, columns[c]] = own[0] | own[1]
                    for side in range(2):
                        a, b = 2 * side, 2 * side + 1
                        best_code[side].append(
                            jnp.where(
                                best[a], value[a], jnp.where(best[b], value[b] * PLANE, 0.0)
                            )
                        )
                for side in range(2):
                    for half in range(2):
                        lower, upper = best_code[side][2 * half : 2 * half + 2]
                        small[side][half].append(jnp.maximum(lower, upper * ROW))
            count = jnp.zeros((SUB, LANES), jnp.int32)
            for side in range(2):
                for half in range(2):
                    for c in range(chunks // 2):
                        even, odd = small[side][half][2 * c : 2 * c + 2]
                        v = jnp.maximum(even * (1 / ODD), odd)
                        cand_send[
                            phase, side, part * part_pairs + 2 * i + half, :, columns[c]
                        ] = v
                        if phase:
                            count = count + jnp.where(v > 0, lone[side], 0)
            if phase:
                tally[2] += count

    def judge(phase, part):
        @pl.loop(0, part_pairs // JUDGED)
        def _(i):
            count = jnp.zeros((SUB, LANES), jnp.int32)
            first = part * part_pairs + JUDGED * i
            for j in range(JUDGED):
                k = 2 * first + 2 * j
                halo = [[0] * chunks, [0] * chunks]
                for side, answer in ((0, HIGH), (1, LOW)):
                    verdicts = []
                    for p in range(chunks // 2):
                        code = cand_recv[phase, side, first + j, :, columns[p]]
                        odd = code >= BASE
                        code = jnp.where(odd, code, code * ODD)
                        row = code >= BASE * ROW
                        code = jnp.where(row, code * (1 / ROW), code)
                        plane = code >= BASE * PLANE
                        code = jnp.where(plane, code * (1 / PLANE), code)
                        bar = [
                            [
                                jnp.where(
                                    plane,
                                    near[side, 1, k + r, :, columns[2 * p + c]],
                                    near[side, 0, k + r, :, columns[2 * p + c]],
                                )
                                for r in range(2)
                            ]
                            for c in range(2)
                        ]
                        bar = [jnp.where(row, b[1], b[0]) for b in bar]
                        alive = code > jnp.where(odd, bar[1], bar[0])
                        verdicts.append(jnp.where(alive, answer, 0))
                        if phase:
                            count = count + jnp.where(alive, 1, 0)
                            continue
                        bit = jnp.where(
                            alive, jnp.where(plane, 2 << (6 * side), 1 << (6 * side)), 0
                        )
                        for c, half in enumerate(
                            (jnp.where(odd, 0, bit), jnp.where(odd, bit, 0))
                        ):
                            halo[0][2 * p + c] |= jnp.where(row, 0, half)
                            halo[1][2 * p + c] |= jnp.where(row, half, 0)
                    resp_send[phase, side, first + j] = verdicts[0] | (verdicts[1] << 16)
                if not phase:
                    for r in range(2):
                        for c in range(chunks):
                            bits[k + r, :, columns[c]] = halo[r][c]
            if phase:
                tally[2] += count

    def allowed(phase, pair):
        word = resp_recv[phase, 0, pair] | resp_recv[phase, 1, pair]
        return word & 0xFFFF, word >> 16

    def settle(part):
        @pl.loop(0, part_pairs // JUDGED)
        def _(i):
            lane = lane_index()
            first = part * part_pairs + JUDGED * i
            for j in range(JUDGED):
                masks = allowed(0, first + j)
                for r in range(2):
                    k = 2 * first + (2 * j + r)
                    row = []
                    for c in range(chunks):
                        row.append(
                            bits[k, :, columns[c]] | (found[k, :, columns[c]] & masks[c // 2])
                        )
                        bits[k, :, columns[c]] = row[c]
                    for c, v in enumerate(lanes5(row, jnp.bitwise_or, lane)):
                        reach[k + HALO, :, columns[c]] = v

    def remove(begin, bodies):
        @pl.loop(0, bodies)
        def _(i):
            lane = lane_index()
            first, second = tally[0], tally[1]
            for block in range(2):
                k = lax.rem(begin + 8 * i + 4 * block, steps)
                tall = [
                    rows5(lambda d: reach[k + (HALO + d), :, columns[c]], jnp.bitwise_or)
                    for c in range(chunks)
                ]
                for r in range(4):
                    rows = [[] for _ in range(depth)]
                    at = pl.ds(pl.multiple_of(SUB * k, SUB) + SUB * r, SUB)
                    for c in range(chunks):
                        own = bits[k + r, :, columns[c]] & (LOW | HIGH)
                        held = tall[c][r]
                        two = held | (held >> 1)
                        cover = (two | (two >> 2) | (held >> 4)) & 15
                        status[c, at, :] = cover | (own << 2)
                        first = first + lax.population_count(own)
                        second = second + lax.population_count(cover)
                        for z in range(depth):
                            value = jnp.where(
                                (cover & (1 << z)) != 0, 0.0, field[z, k + r, :, columns[c]]
                            )
                            field[z, k + r, :, columns[c]] = value
                            rows[z].append(value)
                    for z in range(depth):
                        for c, v in enumerate(lanes5(rows[z], jnp.maximum, lane)):
                            wide[z, k + (HALO + r), :, columns[c]] = v
            tally[0] = first
            tally[1] = second

    def final(part):
        @pl.loop(0, part_pairs // JUDGED)
        def _(i):
            first = part * part_pairs + JUDGED * i
            for j in range(JUDGED):
                masks = allowed(1, first + j)
                for r in range(2):
                    k = 2 * first + (2 * j + r)
                    for c in range(chunks):
                        at = pl.ds(pl.multiple_of(SUB * k, SUB), SUB)
                        held = status[c, at, :]
                        late = ((found[k, :, columns[c]] & masks[c // 2]) << 2) & ~(held << 4)
                        root = ((held | late) >> 4) & 15
                        both = root | ((held & 15 & ~root) << 8)
                        both = (both | (both << 2)) & 0x3333
                        both = (both | (both << 1)) & 0x5555
                        status[c, at, :] = (both & 0xFF) | (both >> 7)

    def offer(phase, part):
        search(phase, part)
        start(cand_send, cand_recv, phase, 2 * phase, part)

    def answer(phase, part):
        finish(cand_send, cand_recv, phase, 2 * phase, part)
        judge(phase, part)
        start(resp_send, resp_recv, phase, 2 * phase + 1, part)

    def confirm(part):
        finish(resp_send, resp_recv, 0, 1, part)
        settle(part)

    @pl.loop(0, chunks)
    def _(piece):
        for z in range(depth):
            pltpu.make_async_copy(
                scores.at[z, :, columns[0]], raw.at[piece, z], in_sem.at[piece, z]
            ).wait()
        turn(piece)

    @pl.loop(0, AHEAD)
    def _(part):
        widen(part)

    pl.semaphore_wait(
        barrier,
        group
        + blocks
        - 2
        + outside[0].astype(jnp.int32)
        + outside[1].astype(jnp.int32),
    )

    @pl.loop(1, AHEAD - 1)
    def _(part):
        offer(0, part)

    @pl.loop(AHEAD, PARTS)
    def _(part):
        widen(part)
        offer(0, part - 1)

    for z in range(depth):
        wrap(wide, (z,))

    @pl.loop(PARTS - 1, PARTS + 1)
    def _(part):
        offer(0, lax.rem(part, PARTS))

    @pl.loop(1, PARTS + 1)
    def _(part):
        answer(0, lax.rem(part, PARTS))

    @pl.loop(1, PARTS)
    def _(part):
        confirm(part)

        @pl.when(part >= 2)
        def _():
            remove(part * part_steps - 4, part_steps // 8)

        @pl.when(part >= 3)
        def _():
            offer(1, part - 1)

    confirm(0)
    wrap(reach, ())
    remove(steps - 4, part_steps // 8 + 1)
    for z in range(depth):
        wrap(wide, (z,))

    @pl.loop(PARTS - 1, PARTS + 2)
    def _(part):
        offer(1, lax.rem(part, PARTS))

    cells = depth * nx * ny
    column = lax.broadcasted_iota(jnp.int32, (1, LANES), 1)
    roots, covered = jnp.sum(tally[0]), jnp.sum(tally[1])
    mine = jnp.where(column == 0, cells - roots, cells - covered)

    @pl.loop(2, PARTS + 2)
    def _(part):
        answer(1, lax.rem(part, PARTS))

    mine = mine - jnp.where(column == 2, jnp.sum(tally[2]), 0)
    cnt_send[...] = mine

    def gather(send, recv, sems, i, device):
        return pltpu.make_async_remote_copy(
            src_ref=send,
            dst_ref=recv.at[i],
            send_sem=sems.at[0, i],
            recv_sem=sems.at[1, i],
            device_id=(device,),
            device_id_type=pl.DeviceIdType.MESH,
        )

    def near_by(i):
        return gather(cnt_send, recv_a, sem_a, i, base + lax.rem(place + i, group))

    def far_off(i):
        return gather(cnt_mid, recv_b, sem_b, i, lax.rem(me + i * group, n))

    @pl.loop(1, group)
    def _(i):
        near_by(i).start()

    def present(c):
        for piece in range(chunks):
            block = jnp.concatenate(
                [
                    status[
                        c, pl.ds(piece * (LANES // steps) + half, steps, stride=SUB), :
                    ]
                    for half in range(LANES // steps)
                ],
                axis=0,
            )
            flat[piece, pl.ds(c, LANES, stride=chunks), :] = block.T

    @pl.loop(1, group)
    def _(i):
        near_by(i).wait()

    subtotal = mine
    for i in range(1, group):
        subtotal = subtotal + recv_a[i]
    cnt_mid[...] = subtotal

    @pl.loop(1, blocks)
    def _(i):
        far_off(i).start()

    @pl.loop(2, PARTS + 2)
    def _(part):
        part = lax.rem(part, PARTS)
        finish(resp_send, resp_recv, 1, 3, part)
        final(part)

    for c in range(chunks):
        present(c)

    @pl.loop(0, nx // SPLIT)
    def _(i):
        here = pl.ds(pl.multiple_of(i * SPLIT, SPLIT), SPLIT)
        for piece in range(chunks):
            word = flat[piece, here, :]
            for z in range(depth):
                decided[z, here, columns[piece]] = (word >> (2 * z)) & 3


    @pl.loop(1, blocks)
    def _(i):
        far_off(i).wait()

    total = subtotal
    for i in range(1, blocks):
        total = total + recv_b[i]
    counts[...] = total


def shards(scores):
    depth, nx, ny = scores.shape
    n = lax.axis_size(AXIS)
    group = math.gcd(GROUP, n)
    vmem = pltpu.VMEM
    steps = nx // SUB
    pairs = steps // 2
    decided, counts = pl.pallas_call(
        functools.partial(kernel, n),
        out_shape=(
            jax.ShapeDtypeStruct((depth, nx, ny), jnp.int32),
            jax.ShapeDtypeStruct((1, LANES), jnp.int32),
        ),
        in_specs=[pl.BlockSpec(memory_space=pltpu.HBM)],
        out_specs=(pl.BlockSpec(memory_space=vmem),) * 2,
        scratch_shapes=[
            vmem((ny // LANES, depth, nx, LANES), jnp.int32),
            vmem((depth, ny // LANES, nx, LANES), jnp.int32),
            vmem((depth, steps, SUB, ny), jnp.float32),
            vmem((depth, steps + 2 * HALO, SUB, ny), jnp.float32),
            vmem((2, 2, steps, SUB, ny), jnp.float32),
            vmem((steps, SUB, ny), jnp.int32),
            vmem((steps + 2 * HALO, SUB, ny), jnp.int32),
            vmem((steps, SUB, ny), jnp.int32),
            vmem((ny // LANES, nx, LANES), jnp.int32),
            vmem((ny // LANES, nx, LANES), jnp.int32),
            vmem((2, 2, pairs, SUB, ny // 2), jnp.float32),
            vmem((2, 2, pairs, SUB, ny // 2), jnp.float32),
            vmem((2, 2, pairs, SUB, ny // 4), jnp.int32),
            vmem((2, 2, pairs, SUB, ny // 4), jnp.int32),
            vmem((3, SUB, LANES), jnp.int32),
            vmem((1, LANES), jnp.int32),
            vmem((1, LANES), jnp.int32),
            vmem((group, 1, LANES), jnp.int32),
            vmem((n // group, 1, LANES), jnp.int32),
            pltpu.SemaphoreType.DMA((ny // LANES, depth)),
            pltpu.SemaphoreType.DMA((4, 2, PARTS)),
            pltpu.SemaphoreType.DMA((4, 2, PARTS)),
            pltpu.SemaphoreType.DMA((2, group)),
            pltpu.SemaphoreType.DMA((2, n // group)),
        ],
        compiler_params=pltpu.CompilerParams(
            collective_id=0, has_side_effects=True, vmem_limit_bytes=48 * 1024 * 1024
        ),
    )(scores)
    return decided, counts[0, :3]


def solution(mesh):
    return jax.shard_map(
        shards,
        mesh=mesh,
        in_specs=(P(AXIS, None, None),),
        out_specs=(P(AXIS, None, None), P()),
        check_vma=False,
    )
```

```python
import functools
import math

import jax
import jax.numpy as jnp
from jax import lax
from jax.experimental import pallas as pl
from jax.experimental.pallas import tpu as pltpu
from jax.sharding import PartitionSpec as P


AXIS = "gz"
SUB = 8
LANES = 128
PARTS = 8
AHEAD = 6
HALO = 2
GROUP = 8
JUDGED = 4
SPLIT = 32
LOW = 0x0C
HIGH = 0x30
BASE = 2.0**23
PLANE = 2.0**16
ROW = 2.0**32
ODD = 2.0**64


def roll(x, shift, axis):
    return pltpu.roll(x, shift % x.shape[axis], axis)


def lane_index():
    return lax.broadcasted_iota(jnp.int32, (SUB, LANES), 1)


def encode(score):
    value = ((score & ((1 << 23) - 1)) | (1 << 23)).astype(jnp.float32)
    scale = lax.shift_left(jnp.ones_like(score), lax.shift_right_logical(score, 23))
    return value * scale.astype(jnp.float32)


def lanes5(x, op, lane):
    blank = jnp.zeros_like(x[0])
    low, high = op(x[0], x[1]), op(x[2], x[3])
    whole = op(low, high)

    def before(v):
        return jnp.where(lane == 0, blank, roll(v, 1, 1))

    def after(v):
        return jnp.where(lane == LANES - 1, blank, roll(v, -1, 1))

    return [
        op(op(low, x[2]), before(high)),
        op(whole, before(x[3])),
        op(whole, after(x[0])),
        op(op(x[1], high), after(low)),
    ]


def rows5(load, op):
    x = {d: load(d) for d in range(-2, 6)}
    middle = op(x[1], x[2])
    left, right = op(x[0], middle), op(middle, x[3])
    left, right = op(x[-1], left), op(right, x[4])
    return [op(left, x[-2]), op(left, x[3]), op(x[0], right), op(right, x[5])]


def kernel(
    n, scores, decided, counts, raw, turned, field, wide, near, bits,
    reach, found, status, flat, cand_send, cand_recv, resp_send, resp_recv, tally, cnt_send, cnt_mid,
    recv_a, recv_b, in_sem, send_sem, recv_sem, sem_a, sem_b,
):
    depth, nx, ny = scores.shape
    chunks = ny // LANES
    steps = nx // SUB
    part_steps = steps // PARTS
    part_pairs = part_steps // 2
    group = math.gcd(GROUP, n)
    blocks = n // group
    me = lax.axis_index(AXIS)
    has = (me > 0, me < n - 1)
    lone = tuple(jnp.where(h, 0, 1).astype(jnp.int32) for h in has)
    columns = [slice(c * LANES, (c + 1) * LANES) for c in range(chunks)]

    def fetch(piece, z):
        return pltpu.make_async_copy(
            scores.at[z, :, columns[piece]], raw.at[piece, z], in_sem.at[piece, z]
        )

    for piece in range(chunks):
        for z in range(depth):
            fetch(piece, z).start()

    barrier = pltpu.get_barrier_semaphore()

    def greet(device):
        pl.semaphore_signal(
            barrier, inc=1, device_id=(device,), device_id_type=pl.DeviceIdType.MESH
        )

    place = lax.rem(me, group)
    base = me - place

    @pl.loop(1, group)
    def _(i):
        greet(base + lax.rem(place + i, group))

    @pl.loop(1, blocks)
    def _(i):
        greet(lax.rem(me + i * group, n))

    outside = (has[0] & (place == 0), has[1] & (place == group - 1))
    for side in range(2):

        @pl.when(outside[side])
        def _():
            greet(me + (1 if side else -1))

    tally[...] = jnp.zeros_like(tally)
    for side, mask in ((0, LOW), (1, HIGH)):

        @pl.when(jnp.logical_not(has[side]))
        def _():
            for phase in range(2):
                cand_recv[phase, side] = jnp.zeros(cand_recv.shape[2:], jnp.float32)
                resp_recv[phase, side] = jnp.full(
                    resp_recv.shape[2:], mask | mask << 16, jnp.int32
                )

    def wrap(ref, index):
        row = lax.broadcasted_iota(jnp.int32, (SUB, ny), 0)
        zero = jnp.zeros((SUB, ny), ref.dtype)
        for d in range(HALO):
            above = ref[index + (steps + d,)]
            ref[index + (d,)] = jnp.where(row == 0, zero, roll(above, 1, 0))
            below = ref[index + (HALO + d,)]
            ref[index + (HALO + steps + d,)] = jnp.where(
                row == SUB - 1, zero, roll(below, -1, 0)
            )

    def exchange(send, recv, phase, step, side, part, arrival):
        rows = pl.ds(part * part_pairs, part_pairs)
        there = arrival if arrival is not None else 1 - side
        return pltpu.make_async_remote_copy(
            src_ref=send.at[phase, side, rows],
            dst_ref=recv.at[phase, there, rows],
            send_sem=send_sem.at[step, side, part],
            recv_sem=recv_sem.at[step, there, part],
            device_id=(me + (1 if side else -1),),
            device_id_type=pl.DeviceIdType.MESH,
        )

    def start(send, recv, phase, step, part):
        for side in range(2):

            @pl.when(has[side])
            def _():
                exchange(send, recv, phase, step, side, part, None).start()

    def finish(send, recv, phase, step, part):
        for side in range(2):

            @pl.when(has[side])
            def _():
                exchange(send, recv, phase, step, side, part, None).wait_send()
                exchange(send, recv, phase, step, side, part, side).wait_recv()

    def turn(piece):
        for z in range(depth):
            for c in range(chunks):
                block = raw[piece, z, pl.ds(c, LANES, stride=chunks), :].T
                for half in range(LANES // steps):
                    turned[
                        z, c, pl.ds(piece * (LANES // steps) + half, steps, stride=SUB), :
                    ] = block[half * steps : (half + 1) * steps]

    def widen(part):
        lane = lane_index()
        k = part * part_steps
        for r in range(part_steps):
            for z in range(depth):
                row = []
                for c in range(chunks):
                    score = turned[
                        z, c, pl.ds(pl.multiple_of(SUB * k, SUB) + SUB * r, SUB), :
                    ]
                    value = encode(score)
                    field[z, k + r, :, columns[c]] = value
                    row.append(value)
                for c, v in enumerate(lanes5(row, jnp.maximum, lane)):
                    wide[z, k + (HALO + r), :, columns[c]] = v

    def search(phase, part):
        @pl.loop(0, part_pairs // 2)
        def _(i):
            k = part * part_steps + 4 * i
            small = [[[], []], [[], []]]
            for c in range(chunks):
                tall = [
                    rows5(lambda d: wide[z, k + (HALO + d), :, columns[c]], jnp.maximum)
                    for z in range(depth)
                ]
                best_code = ([], [])
                for r in range(4):
                    w = [tall[z][r] for z in range(depth)]
                    low, high = jnp.maximum(w[0], w[1]), jnp.maximum(w[2], w[3])
                    near[0, 0, k + r, :, columns[c]] = w[0]
                    near[0, 1, k + r, :, columns[c]] = low
                    near[1, 0, k + r, :, columns[c]] = high
                    near[1, 1, k + r, :, columns[c]] = w[3]
                    whole = jnp.maximum(low, high)
                    peak = [jnp.maximum(low, w[2]), whole, whole, jnp.maximum(w[1], high)]
                    value = [field[z, k + r, :, columns[c]] for z in range(depth)]
                    best = [value[z] == peak[z] for z in range(depth)]
                    own = [
                        jnp.where(best[z], 4 << z, jnp.where(best[z + 1], 8 << z, 0))
                        for z in (0, 2)
                    ]
                    found[k + r, :, columns[c]] = own[0] | own[1]
                    for side in range(2):
                        a, b = 2 * side, 2 * side + 1
                        best_code[side].append(
                            jnp.where(
                                best[a], value[a], jnp.where(best[b], value[b] * PLANE, 0.0)
                            )
                        )
                for side in range(2):
                    for half in range(2):
                        lower, upper = best_code[side][2 * half : 2 * half + 2]
                        small[side][half].append(jnp.maximum(lower, upper * ROW))
            count = jnp.zeros((SUB, LANES), jnp.int32)
            for side in range(2):
                for half in range(2):
                    for c in range(chunks // 2):
                        even, odd = small[side][half][2 * c : 2 * c + 2]
                        v = jnp.maximum(even * (1 / ODD), odd)
                        cand_send[
                            phase, side, part * part_pairs + 2 * i + half, :, columns[c]
                        ] = v
                        if phase:
                            count = count + jnp.where(v > 0, lone[side], 0)
            if phase:
                tally[2] += count

    def judge(phase, part):
        @pl.loop(0, part_pairs // JUDGED)
        def _(i):
            count = jnp.zeros((SUB, LANES), jnp.int32)
            first = part * part_pairs + JUDGED * i
            for j in range(JUDGED):
                k = 2 * first + 2 * j
                halo = [[0] * chunks, [0] * chunks]
                for side, answer in ((0, HIGH), (1, LOW)):
                    verdicts = []
                    for p in range(chunks // 2):
                        code = cand_recv[phase, side, first + j, :, columns[p]]
                        odd = code >= BASE
                        code = jnp.where(odd, code, code * ODD)
                        row = code >= BASE * ROW
                        code = jnp.where(row, code * (1 / ROW), code)
                        plane = code >= BASE * PLANE
                        code = jnp.where(plane, code * (1 / PLANE), code)
                        bar = [
                            [
                                jnp.where(
                                    plane,
                                    near[side, 1, k + r, :, columns[2 * p + c]],
                                    near[side, 0, k + r, :, columns[2 * p + c]],
                                )
                                for r in range(2)
                            ]
                            for c in range(2)
                        ]
                        bar = [jnp.where(row, b[1], b[0]) for b in bar]
                        alive = code > jnp.where(odd, bar[1], bar[0])
                        verdicts.append(jnp.where(alive, answer, 0))
                        if phase:
                            count = count + jnp.where(alive, 1, 0)
                            continue
                        bit = jnp.where(
                            alive, jnp.where(plane, 2 << (6 * side), 1 << (6 * side)), 0
                        )
                        for c, half in enumerate(
                            (jnp.where(odd, 0, bit), jnp.where(odd, bit, 0))
                        ):
                            halo[0][2 * p + c] |= jnp.where(row, 0, half)
                            halo[1][2 * p + c] |= jnp.where(row, half, 0)
                    resp_send[phase, side, first + j] = verdicts[0] | (verdicts[1] << 16)
                if not phase:
                    for r in range(2):
                        for c in range(chunks):
                            bits[k + r, :, columns[c]] = halo[r][c]
            if phase:
                tally[2] += count

    def allowed(phase, pair):
        word = resp_recv[phase, 0, pair] | resp_recv[phase, 1, pair]
        return word & 0xFFFF, word >> 16

    def settle(part):
        @pl.loop(0, part_pairs // JUDGED)
        def _(i):
            lane = lane_index()
            first = part * part_pairs + JUDGED * i
            for j in range(JUDGED):
                masks = allowed(0, first + j)
                for r in range(2):
                    k = 2 * first + (2 * j + r)
                    row = []
                    for c in range(chunks):
                        row.append(
                            bits[k, :, columns[c]] | (found[k, :, columns[c]] & masks[c // 2])
                        )
                        bits[k, :, columns[c]] = row[c]
                    for c, v in enumerate(lanes5(row, jnp.bitwise_or, lane)):
                        reach[k + HALO, :, columns[c]] = v

    def remove(begin, bodies):
        @pl.loop(0, bodies)
        def _(i):
            lane = lane_index()
            for block in range(2):
                k = lax.rem(begin + 8 * i + 4 * block, steps)
                tall = [
                    rows5(lambda d: reach[k + (HALO + d), :, columns[c]], jnp.bitwise_or)
                    for c in range(chunks)
                ]
                for r in range(4):
                    rows = [[] for _ in range(depth)]
                    at = pl.ds(pl.multiple_of(SUB * k, SUB) + SUB * r, SUB)
                    for c in range(chunks):
                        own = bits[k + r, :, columns[c]] & (LOW | HIGH)
                        held = tall[c][r]
                        two = held | (held >> 1)
                        cover = (two | (two >> 2) | (held >> 4)) & 15
                        status[c, at, :] = cover | (own << 2)
                        for z in range(depth):
                            value = jnp.where(
                                (cover & (1 << z)) != 0, 0.0, field[z, k + r, :, columns[c]]
                            )
                            field[z, k + r, :, columns[c]] = value
                            rows[z].append(value)
                    for z in range(depth):
                        for c, v in enumerate(lanes5(rows[z], jnp.maximum, lane)):
                            wide[z, k + (HALO + r), :, columns[c]] = v

    def final(part):
        @pl.loop(0, part_pairs // JUDGED)
        def _(i):
            first = part * part_pairs + JUDGED * i
            for j in range(JUDGED):
                masks = allowed(1, first + j)
                for r in range(2):
                    k = 2 * first + (2 * j + r)
                    for c in range(chunks):
                        at = pl.ds(pl.multiple_of(SUB * k, SUB), SUB)
                        held = status[c, at, :]
                        late = ((found[k, :, columns[c]] & masks[c // 2]) << 2) & ~(held << 4)
                        root = ((held | late) >> 4) & 15
                        both = root | ((held & 15 & ~root) << 8)
                        both = (both | (both << 2)) & 0x3333
                        both = (both | (both << 1)) & 0x5555
                        status[c, at, :] = (both & 0xFF) | (both >> 7)

    def offer(phase, part):
        search(phase, part)
        start(cand_send, cand_recv, phase, 2 * phase, part)

    def answer(phase, part):
        finish(cand_send, cand_recv, phase, 2 * phase, part)
        judge(phase, part)
        start(resp_send, resp_recv, phase, 2 * phase + 1, part)

    def confirm(part):
        finish(resp_send, resp_recv, 0, 1, part)
        settle(part)

    @pl.loop(0, chunks)
    def _(piece):
        for z in range(depth):
            pltpu.make_async_copy(
                scores.at[z, :, columns[0]], raw.at[piece, z], in_sem.at[piece, z]
            ).wait()
        turn(piece)

    @pl.loop(0, AHEAD)
    def _(part):
        widen(part)

    pl.semaphore_wait(
        barrier,
        group
        + blocks
        - 2
        + outside[0].astype(jnp.int32)
        + outside[1].astype(jnp.int32),
    )

    @pl.loop(1, AHEAD - 1)
    def _(part):
        offer(0, part)

    @pl.loop(AHEAD, PARTS)
    def _(part):
        widen(part)
        offer(0, part - 1)

    for z in range(depth):
        wrap(wide, (z,))

    @pl.loop(PARTS - 1, PARTS + 1)
    def _(part):
        offer(0, lax.rem(part, PARTS))

    @pl.loop(1, PARTS + 1)
    def _(part):
        answer(0, lax.rem(part, PARTS))

    @pl.loop(1, PARTS)
    def _(part):
        confirm(part)

        @pl.when(part >= 2)
        def _():
            remove(part * part_steps - 4, part_steps // 8)

        @pl.when(part >= 3)
        def _():
            offer(1, part - 1)

    confirm(0)
    wrap(reach, ())
    remove(steps - 4, part_steps // 8 + 1)
    for z in range(depth):
        wrap(wide, (z,))

    @pl.loop(PARTS - 1, PARTS + 2)
    def _(part):
        offer(1, lax.rem(part, PARTS))

    @pl.loop(0, nx // SPLIT)
    def _(i):
        first, second = tally[0], tally[1]
        for r in range(0, SPLIT, SUB):
            at = pl.ds(pl.multiple_of(i * SPLIT, SPLIT) + r, SUB)
            for c in range(chunks):
                first = first + lax.population_count(status[c, at, :] >> 4)
                second = second + lax.population_count(status[c, at, :] & 15)
        tally[0] = first
        tally[1] = second

    cells = depth * nx * ny
    column = lax.broadcasted_iota(jnp.int32, (1, LANES), 1)
    roots, covered = jnp.sum(tally[0]), jnp.sum(tally[1])
    mine = jnp.where(column == 0, cells - roots, cells - covered)

    @pl.loop(2, PARTS + 2)
    def _(part):
        answer(1, lax.rem(part, PARTS))

    mine = mine - jnp.where(column == 2, jnp.sum(tally[2]), 0)
    cnt_send[...] = mine

    def gather(send, recv, sems, i, device):
        return pltpu.make_async_remote_copy(
            src_ref=send,
            dst_ref=recv.at[i],
            send_sem=sems.at[0, i],
            recv_sem=sems.at[1, i],
            device_id=(device,),
            device_id_type=pl.DeviceIdType.MESH,
        )

    def near_by(i):
        return gather(cnt_send, recv_a, sem_a, i, base + lax.rem(place + i, group))

    def far_off(i):
        return gather(cnt_mid, recv_b, sem_b, i, lax.rem(me + i * group, n))

    @pl.loop(1, group)
    def _(i):
        near_by(i).start()

    def present(c):
        for piece in range(chunks):
            block = jnp.concatenate(
                [
                    status[
                        c, pl.ds(piece * (LANES // steps) + half, steps, stride=SUB), :
                    ]
                    for half in range(LANES // steps)
                ],
                axis=0,
            )
            flat[piece, pl.ds(c, LANES, stride=chunks), :] = block.T

    @pl.loop(1, group)
    def _(i):
        near_by(i).wait()

    subtotal = mine
    for i in range(1, group):
        subtotal = subtotal + recv_a[i]
    cnt_mid[...] = subtotal

    @pl.loop(1, blocks)
    def _(i):
        far_off(i).start()

    @pl.loop(2, PARTS + 2)
    def _(part):
        part = lax.rem(part, PARTS)
        finish(resp_send, resp_recv, 1, 3, part)
        final(part)

    for c in range(chunks):
        present(c)

    @pl.loop(0, nx // SPLIT)
    def _(i):
        here = pl.ds(pl.multiple_of(i * SPLIT, SPLIT), SPLIT)
        for piece in range(chunks):
            word = flat[piece, here, :]
            for z in range(depth):
                decided[z, here, columns[piece]] = (word >> (2 * z)) & 3


    @pl.loop(1, blocks)
    def _(i):
        far_off(i).wait()

    total = subtotal
    for i in range(1, blocks):
        total = total + recv_b[i]
    counts[...] = total


def shards(scores):
    depth, nx, ny = scores.shape
    n = lax.axis_size(AXIS)
    group = math.gcd(GROUP, n)
    vmem = pltpu.VMEM
    steps = nx // SUB
    pairs = steps // 2
    decided, counts = pl.pallas_call(
        functools.partial(kernel, n),
        out_shape=(
            jax.ShapeDtypeStruct((depth, nx, ny), jnp.int32),
            jax.ShapeDtypeStruct((1, LANES), jnp.int32),
        ),
        in_specs=[pl.BlockSpec(memory_space=pltpu.HBM)],
        out_specs=(pl.BlockSpec(memory_space=vmem),) * 2,
        scratch_shapes=[
            vmem((ny // LANES, depth, nx, LANES), jnp.int32),
            vmem((depth, ny // LANES, nx, LANES), jnp.int32),
            vmem((depth, steps, SUB, ny), jnp.float32),
            vmem((depth, steps + 2 * HALO, SUB, ny), jnp.float32),
            vmem((2, 2, steps, SUB, ny), jnp.float32),
            vmem((steps, SUB, ny), jnp.int32),
            vmem((steps + 2 * HALO, SUB, ny), jnp.int32),
            vmem((steps, SUB, ny), jnp.int32),
            vmem((ny // LANES, nx, LANES), jnp.int32),
            vmem((ny // LANES, nx, LANES), jnp.int32),
            vmem((2, 2, pairs, SUB, ny // 2), jnp.float32),
            vmem((2, 2, pairs, SUB, ny // 2), jnp.float32),
            vmem((2, 2, pairs, SUB, ny // 4), jnp.int32),
            vmem((2, 2, pairs, SUB, ny // 4), jnp.int32),
            vmem((3, SUB, LANES), jnp.int32),
            vmem((1, LANES), jnp.int32),
            vmem((1, LANES), jnp.int32),
            vmem((group, 1, LANES), jnp.int32),
            vmem((n // group, 1, LANES), jnp.int32),
            pltpu.SemaphoreType.DMA((ny // LANES, depth)),
            pltpu.SemaphoreType.DMA((4, 2, PARTS)),
            pltpu.SemaphoreType.DMA((4, 2, PARTS)),
            pltpu.SemaphoreType.DMA((2, group)),
            pltpu.SemaphoreType.DMA((2, n // group)),
        ],
        compiler_params=pltpu.CompilerParams(
            collective_id=0, has_side_effects=True, vmem_limit_bytes=48 * 1024 * 1024
        ),
    )(scores)
    return decided, counts[0, :3]


def solution(mesh):
    return jax.shard_map(
        shards,
        mesh=mesh,
        in_specs=(P(AXIS, None, None),),
        out_specs=(P(AXIS, None, None), P()),
        check_vma=False,
    )
```
